32 devices in a mesh: dp: 8 (over z, y), tp: 4 (over x, core).
Axes of the slice: x: 2, y: 2, z: 4, core: 2. Of those that a mesh axis runs over, the one named last changes fastest.
Arguments:
- tokens: bfloat16 [16384, 768], P('dp'), may hold values from -6 to 6
- box_coords: int32 [2, 16384], P(None, 'dp'), may hold values from 0 to 999
- page_lengths: int32 [32, 4], P('dp'), may hold values from 1 to 320, 512 in all within a row
- query_weight: bfloat16 [768, 768], P(None, 'tp'), may hold values from -0.4375 to 0.4375
- key_weight: bfloat16 [768, 768], P(None, 'tp'), may hold values from -0.21875 to 0.21875
- value_weight: bfloat16 [768, 768], P(None, 'tp'), may hold values from -0.21875 to 0.21875
- box_query: bfloat16 [768, 768], P(None, 'tp'), may hold values from -0.4375 to 0.4375
- box_key: bfloat16 [768, 768], P(None, 'tp'), may hold values from -0.21875 to 0.21875
- out_weight: bfloat16 [768, 768], P('tp'), may hold values from -1.75 to 1.75
- first_gain: bfloat16 [768], replicated, may hold values from 0.5 to 1.5
- first_shift: bfloat16 [768], replicated, may hold values from -3 to 3
- widen_weight: bfloat16 [768, 3072], P(None, 'tp'), may hold values from -0.21875 to 0.21875
- widen_bias: bfloat16 [3072], P('tp'), may hold values from -3 to 3
- narrow_weight: bfloat16 [3072, 768], P('tp'), may hold values from -0.109375 to 0.109375
- second_gain: bfloat16 [768], replicated, may hold values from 0.5 to 1.5
- second_shift: bfloat16 [768], replicated, may hold values from -3 to 3
- cotangent: bfloat16 [16384, 768], P('dp'), may hold values from -6 to 6
Outputs:
- output: float32 [16384, 768], P('dp')
- input_grad: float32 [16384, 768], P('dp')
- query_grad: float32 [768, 768], P(None, 'tp')
- key_grad: float32 [768, 768], P(None, 'tp')
- value_grad: float32 [768, 768], P(None, 'tp')
- box_query_grad: float32 [768, 768], P(None, 'tp')
- box_key_grad: float32 [768, 768], P(None, 'tp')
- out_grad: float32 [768, 768], P('tp')
- first_gain_grad: float32 [768], replicated
- first_shift_grad: float32 [768], replicated
- widen_grad: float32 [768, 3072], P(None, 'tp')
- widen_bias_grad: float32 [3072], P('tp')
- narrow_grad: float32 [3072, 768], P('tp')
- second_gain_grad: float32 [768], replicated
- second_shift_grad: float32 [768], replicated
The draws below stay inside these ranges and needn't reach their ends.
Inputs may be any that keep to these rules, and one draw needn't show every extreme that they name: `page_lengths`: the 4 page lengths of each row sum to 512, and the longest page of each row has 320 tokens.
All inputs are finite; a program needn't handle non-finite values.
Results may differ from the reference program's by a relative error of at most 0.017.
Values sent between devices are 32-bit elements; how exact they have to be, the bound alone decides.
A program may use at most 192 MiB of HBM per device.

```python
import math
import jax
import jax.numpy as jnp
import numpy as np
from jax import lax

D = 768
HEADS = 12
HEAD = 64
FF = 3072
SEQ = 512
PAGES = 4
MOST_PAGE = 320
ROWS = 32
TOKENS = 16384


def place_ends(drawn, stream_key, low, largest):
    extent = drawn.shape
    spot = [jax.random.randint(jax.random.fold_in(stream_key, axis), (), 0, extent[axis]) for axis in range(len(extent))]
    drawn = drawn.at[tuple(spot)].set(low)
    longest = extent.index(max(extent))
    spot[longest] = (spot[longest] + 1) % extent[longest]
    return drawn.at[tuple(spot)].set(largest)


def steps_of(key, extent, cuts, low, top_value):
    level, own = 1.0, jax.random.fold_in(key, 6)
    for axis_at, blocks in cuts:
        draws = jnp.exp(jax.random.uniform(jax.random.fold_in(own, axis_at), (blocks,), jnp.float32, low / len(cuts), top_value / len(cuts)))
        level = level * jnp.repeat(draws, extent[axis_at] // blocks).reshape([-1 if axis == axis_at else 1 for axis in range(len(extent))])
    return level


def length_profile(amount, total, reach, skew):
    portions = [(1 << 20) // math.isqrt(rank ** skew) + 1 for rank in range(2, amount + 1)]
    spare, given = total - reach - (amount - 1), [1] * (amount - 1)
    while spare > 0:
        free = [i for i in range(amount - 1) if given[i] < reach]
        whole, left = sum([portions[i] for i in free]), spare
        for i in free:
            extra = min(reach - given[i], max(1, left * portions[i] // whole), spare)
            given[i] = given[i] + extra
            spare = spare - extra
    return np.array([reach] + given)


def uneven(rng, count, total, reach, slope):
    if count == 2:
        one = jax.random.randint(rng, (), max(1, total - reach), min(reach, total - 1) + 1)
        return jnp.stack([one, total - one])
    tallies = jnp.asarray(length_profile(count, total, reach, slope), jnp.int32)
    couples = (count - 1) // 2
    donor, sink = tallies[1:1 + 2 * couples:2], tallies[2:2 + 2 * couples:2]
    margin = jnp.minimum(donor - 1, reach - sink)
    passed = jax.random.randint(jax.random.fold_in(rng, 1), (couples,), 0, 1 << 20) % (margin + 1)
    tallies = tallies.at[1:1 + 2 * couples:2].set(donor - passed).at[2:2 + 2 * couples:2].set(sink + passed)
    return tallies[jax.random.permutation(jax.random.fold_in(rng, 2), count)]


def scatter_about(rng, extent, scale, limit, cuts=(), kind=jnp.bfloat16):
    drawn = jax.random.normal(rng, extent, jnp.float32) * scale
    if len(cuts) > 0:
        drawn = steps_of(rng, extent, cuts, -0.22, 0.18) * drawn
    return jnp.clip(drawn, min=-limit, max=limit).astype(kind)


def setup_inputs(seed: int = 0) -> dict:
    key_list = jax.random.split(jax.random.key(seed), 18)
    tokens = scatter_about(key_list[0], (TOKENS, D), 1.0, 6.0, ((0, 8),))
    box_coords = place_ends(jax.random.randint(key_list[1], (2, TOKENS), 0, 1000), jax.random.fold_in(key_list[1], 1), 0, 999).astype(jnp.int32)
    page_lengths = jax.vmap(lambda own: uneven(own, PAGES, SEQ, MOST_PAGE, 2))(jax.random.split(key_list[2], ROWS)).reshape((ROWS, PAGES)).astype(jnp.int32)
    query_weight = scatter_about(key_list[3], (D, D), (D // 4) ** -0.5, 0.4375, ((1, 4),))
    key_weight = scatter_about(key_list[4], (D, D), D ** -0.5, 0.21875, ((1, 4),))
    value_weight = scatter_about(key_list[5], (D, D), D ** -0.5, 0.21875, ((1, 4),))
    box_query = scatter_about(key_list[6], (D, D), (D // 4) ** -0.5, 0.4375, ((1, 4),))
    box_key = scatter_about(key_list[7], (D, D), D ** -0.5, 0.21875, ((1, 4),))
    out_weight = scatter_about(key_list[8], (D, D), (D // 64) ** -0.5, 1.75, ((0, 4),))
    first_gain = jnp.clip(1.0 + 0.1 * jax.random.normal(key_list[9], (D,), jnp.float32), 0.5, 1.5).astype(jnp.bfloat16)
    first_shift = scatter_about(key_list[10], (D,), 0.5, 3.0)
    widen_weight = scatter_about(key_list[11], (D, FF), D ** -0.5, 0.21875, ((1, 4),))
    widen_bias = scatter_about(key_list[12], (FF,), 0.5, 3.0, ((0, 4),))
    narrow_weight = scatter_about(key_list[13], (FF, D), FF ** -0.5, 0.109375, ((0, 4),))
    second_gain = jnp.clip(1.0 + 0.1 * jax.random.normal(key_list[14], (D,), jnp.float32), 0.5, 1.5).astype(jnp.bfloat16)
    second_shift = scatter_about(key_list[15], (D,), 0.5, 3.0)
    cotangent = scatter_about(key_list[16], (TOKENS, D), 1.0, 6.0, ((0, 8),))
    return {"tokens": tokens, "box_coords": box_coords, "page_lengths": page_lengths, "query_weight": query_weight, "key_weight": key_weight, "value_weight": value_weight, "box_query": box_query, "box_key": box_key, "out_weight": out_weight, "first_gain": first_gain, "first_shift": first_shift, "widen_weight": widen_weight, "widen_bias": widen_bias, "narrow_weight": narrow_weight, "second_gain": second_gain, "second_shift": second_shift, "cotangent": cotangent}


@jax.custom_vjp
def low(v):
    return lax.optimization_barrier(v.astype(jnp.bfloat16)).astype(jnp.float32)

@jax.custom_vjp
def low_back(v):
    return v

def low_keep(v):
    return (low(v), None)

def low_pass(kept, grad):
    return (grad,)

def back_keep(v):
    return (v, None)

def back_low(kept, grad):
    return (low(grad),)
low.defvjp(low_keep, low_pass)
low_back.defvjp(back_keep, back_low)
EPSILON = 1e-05
HIGHEST = lax.Precision.HIGHEST

def product(left, right):
    return jnp.dot(left, right, precision=HIGHEST, preferred_element_type=jnp.float32)

def rounded(value):
    return low_back(low(value))

def layer_norm(values, gain, shift):
    centre = lax.optimization_barrier(jnp.mean(values, axis=-1, keepdims=True))
    centred = values - centre
    spread = lax.optimization_barrier(jnp.mean(centred * centred, axis=-1, keepdims=True))
    return centred * lax.rsqrt(spread + EPSILON) * gain + shift

def page_table(lengths, length):
    ends = jnp.cumsum(lengths, axis=1)
    places = jnp.arange(length, dtype=jnp.int32)
    return lax.optimization_barrier(jnp.sum((ends[:, None, :] <= places[None, :, None]).astype(jnp.int32), axis=2))

def box_embed(coords, width):
    quarter = width // 4
    steps = jnp.arange(quarter).astype(jnp.float32)
    freq = jnp.exp(-math.log(10000.0) * steps / quarter)
    across = coords[0].astype(jnp.float32)[:, None] * freq[None, :]
    downward = coords[1].astype(jnp.float32)[:, None] * freq[None, :]
    return jnp.concatenate([jnp.sin(across), jnp.cos(across), jnp.sin(downward), jnp.cos(downward)], axis=1)

def attend_row(items):
    query_cat, key_cat, values, page_row = items
    scale = 1.0 / math.sqrt(query_cat.shape[-1])
    scores = low_back(jnp.einsum('qhd,khd->hqk', query_cat, key_cat, precision=HIGHEST) * scale)
    allowed = page_row[:, None] == page_row[None, :]
    scores = jnp.where(allowed[None], scores, -1e+30)
    totals = jax.nn.logsumexp(scores, axis=-1, keepdims=True)
    weights = low(jnp.exp(scores - totals))
    return jnp.einsum('hqk,khd->qhd', weights, values, precision=HIGHEST)

def forward(inputs, box, pages, params):
    query_weight, key_weight, value_weight, box_query, box_key, out_weight, first_gain, first_shift, widen_weight, widen_bias, narrow_weight, second_gain, second_shift = params
    rows = pages.shape[0]
    length = pages.shape[1]

    def heads_of(matrix):
        return matrix.reshape(rows, length, HEADS, HEAD)
    queries = heads_of(rounded(product(inputs, query_weight)))
    keys = heads_of(rounded(product(inputs, key_weight)))
    values = heads_of(rounded(product(inputs, value_weight)))
    box_queries = heads_of(rounded(product(box, box_query)))
    box_keys = heads_of(rounded(product(box, box_key)))
    query_cat = jnp.concatenate([queries, box_queries], axis=3)
    key_cat = jnp.concatenate([keys, box_keys], axis=3)
    mixed = lax.map(jax.checkpoint(attend_row), (query_cat, key_cat, values, pages))
    mixed = rounded(mixed.reshape(rows * length, HEADS * HEAD))
    attended = low_back(product(mixed, out_weight))
    hidden = layer_norm(inputs + attended, first_gain, first_shift)
    pre_act = low_back(product(low(hidden), widen_weight) + widen_bias)
    acted = low(jax.nn.gelu(pre_act, approximate=True))
    branch = low_back(product(acted, narrow_weight))
    return layer_norm(hidden + branch, second_gain, second_shift)

def reference(tokens, box_coords, page_lengths, query_weight, key_weight, value_weight, box_query, box_key, out_weight, first_gain, first_shift, widen_weight, widen_bias, narrow_weight, second_gain, second_shift, cotangent):
    params = tuple((weight.astype(jnp.float32) for weight in (query_weight, key_weight, value_weight, box_query, box_key, out_weight, first_gain, first_shift, widen_weight, widen_bias, narrow_weight, second_gain, second_shift)))
    group = math.gcd(ROWS, max(1, 4096 // SEQ))
    count = ROWS // group
    inputs_all = tokens.astype(jnp.float32).reshape(count, group * SEQ, D)
    box_all = low(box_embed(box_coords, D)).reshape(count, group * SEQ, D)
    pages_all = page_table(page_lengths, SEQ).reshape(count, group, SEQ)
    grads_all = cotangent.astype(jnp.float32).reshape(count, group * SEQ, D)

    def one_group(carry, items):
        inputs, box, pages, incoming = items

        def layer(values, weights):
            return forward(values, box, pages, weights)
        result, pull = jax.vjp(layer, inputs, params)
        grad_inputs, grad_params = pull(incoming)
        return (tuple((total + term for total, term in zip(carry, grad_params))), (result, grad_inputs))
    start = tuple((jnp.zeros(weight.shape, jnp.float32) for weight in params))
    grads, (results, grad_inputs) = lax.scan(one_group, start, (inputs_all, box_all, pages_all, grads_all))
    return (results.reshape(TOKENS, D), grad_inputs.reshape(TOKENS, D), grads[0], grads[1], grads[2], grads[3], grads[4], grads[5], grads[6], grads[7], grads[8], grads[9], grads[10], grads[11], grads[12])
```

```python
import functools
import math

import jax
import jax.numpy as jnp
from jax import lax
from jax.sharding import PartitionSpec as P

HEAD = 64


EPSILON = 1e-05


def over_rows(left, right):
    return lax.dot_general(
        left, right, (((0,), (0,)), ((), ())), preferred_element_type=jnp.float32
    )


def along_cols(left, right):
    return lax.dot_general(
        left, right, (((1,), (1,)), ((), ())), preferred_element_type=jnp.float32
    )


def page_table(lengths, length):
    ends = jnp.cumsum(lengths, axis=1)
    places = jnp.arange(length, dtype=jnp.int32)
    return jnp.sum((ends[:, None, :] <= places[None, :, None]).astype(jnp.int32), axis=2)


def box_embed(coords, width):
    quarter = width // 4
    steps = jnp.arange(quarter).astype(jnp.float32)
    freq = jnp.exp(-math.log(10000.0) * steps / quarter)
    across = coords[0].astype(jnp.float32)[:, None] * freq[None, :]
    downward = coords[1].astype(jnp.float32)[:, None] * freq[None, :]
    return jnp.concatenate(
        [jnp.sin(across), jnp.cos(across), jnp.sin(downward), jnp.cos(downward)], axis=1
    )


def norm_forward(values, gain, shift):
    centre = jnp.mean(values, axis=-1, keepdims=True)
    centred = values - centre
    inverse = lax.rsqrt(jnp.mean(centred * centred, axis=-1, keepdims=True) + EPSILON)
    normed = centred * inverse
    return (normed * gain.astype(jnp.float32) + shift.astype(jnp.float32), normed, inverse)


def norm_backward(incoming, normed, inverse, gain):
    scaled = incoming * gain.astype(jnp.float32)
    grad_in = inverse * (
        scaled
        - jnp.mean(scaled, axis=-1, keepdims=True)
        - normed * jnp.mean(scaled * normed, axis=-1, keepdims=True)
    )
    return (grad_in, jnp.sum(incoming * normed, axis=0), jnp.sum(incoming, axis=0))


def row_scores(query_cat, key_cat, page_row):
    scale = 1.0 / math.sqrt(query_cat.shape[-1])
    scores = (
        jnp.einsum("qhd,khd->hqk", query_cat, key_cat, preferred_element_type=jnp.float32) * scale
    )
    allowed = page_row[:, None] == page_row[None, :]
    return (jnp.where(allowed[None], scores, -1e30), scale)


def attend_row(items):
    query_cat, key_cat, values, page_row = items
    scores, scale = row_scores(query_cat, key_cat, page_row)
    totals = jax.nn.logsumexp(scores, axis=-1, keepdims=True)
    weights = jnp.exp(scores - totals).astype(jnp.bfloat16)
    mixed = jnp.einsum("hqk,khd->qhd", weights, values, preferred_element_type=jnp.float32)
    return (mixed.astype(jnp.bfloat16), totals)


def attend_back(items):
    query_cat, key_cat, values, grad_mixed, page_row, totals = items
    scores, scale = row_scores(query_cat, key_cat, page_row)
    probs = jnp.exp(scores - totals)
    probs_low = probs.astype(jnp.bfloat16)
    grad_probs = jnp.einsum("qhd,khd->hqk", grad_mixed, values, preferred_element_type=jnp.float32)
    centre = jnp.sum(probs * grad_probs, axis=-1, keepdims=True)
    grad_scores = (probs * (grad_probs - centre)).astype(jnp.bfloat16)
    grad_query = (
        jnp.einsum("hqk,khd->qhd", grad_scores, key_cat, preferred_element_type=jnp.float32) * scale
    )
    grad_key = (
        jnp.einsum("hqk,qhd->khd", grad_scores, query_cat, preferred_element_type=jnp.float32)
        * scale
    )
    grad_value = jnp.einsum(
        "hqk,qhd->khd", probs_low, grad_mixed, preferred_element_type=jnp.float32
    )
    return (
        grad_query.astype(jnp.bfloat16),
        grad_key.astype(jnp.bfloat16),
        grad_value.astype(jnp.bfloat16),
    )


def trade_cores(value):
    return lax.ppermute(value, "tp", [(place, place ^ 1) for place in range(4)])


def trade_chips(value):
    return lax.ppermute(value, "tp", [(place, place ^ 2) for place in range(4)])


def split_block(value, bit):
    size = value.shape[0] // 2
    return block_at(value, bit, size), block_at(value, 1 - bit, size)


def block_at(value, place, size):
    return lax.dynamic_slice_in_dim(value, place * size, size, axis=0)


def trade_dp(value, count, bit):
    return lax.ppermute(value, "dp", [(place, place ^ bit) for place in range(count)])


def sum_over_dp(value, count, order):
    if count != 8:
        return lax.psum(value, "dp")
    me = lax.axis_index("dp")
    for bit in order:
        keep, send = split_block(value, (me // bit) % 2)
        value = keep + trade_dp(send, count, bit)
    for bit in order[::-1]:
        got = trade_dp(value, count, bit)
        side = (me // bit) % 2
        value = jnp.concatenate(
            [jnp.where(side == 0, value, got), jnp.where(side == 0, got, value)], axis=0
        )
    return value


def small_sum_over_dp(value, count):
    if count & (count - 1):
        return lax.psum(value, "dp")
    bit = 1
    while bit < count:
        value = value + lax.ppermute(
            value, "dp", [(place, place ^ bit) for place in range(count)]
        )
        bit *= 2
    return value


def attn_forward(inputs, box_low, pages, params):
    query_weight, key_weight, value_weight, box_query, box_key, out_weight = params[:6]
    rows, length = pages.shape
    local_heads = query_weight.shape[1] // HEAD

    def project(left, right):
        matrix = jnp.dot(left, right, preferred_element_type=jnp.float32).astype(jnp.bfloat16)
        return matrix.reshape(rows, length, local_heads, HEAD)

    query_cat = jnp.concatenate(
        [project(inputs, query_weight), project(box_low, box_query)], axis=3
    )
    key_cat = jnp.concatenate([project(inputs, key_weight), project(box_low, box_key)], axis=3)
    values = project(inputs, value_weight)
    mixed, totals = [], []
    for row in range(rows):
        one, total = attend_row((query_cat[row], key_cat[row], values[row], pages[row]))
        mixed.append(one.reshape(length, local_heads * HEAD))
        totals.append(total)
    parts = [jnp.dot(one, out_weight, preferred_element_type=jnp.float32) for one in mixed]
    return parts, (query_cat, key_cat, values, mixed, totals)


def ffn_forward(inputs, attended, params):
    first_gain, first_shift, widen_weight, widen_bias, narrow_weight = params[6:11]
    hidden, normed, inverse = norm_forward(
        inputs.astype(jnp.float32) + attended, first_gain, first_shift
    )
    hidden_low = hidden.astype(jnp.bfloat16)
    pre_act = jnp.dot(
        hidden_low, widen_weight, preferred_element_type=jnp.float32
    ) + widen_bias.astype(jnp.float32)
    acted = jax.nn.gelu(pre_act, approximate=True).astype(jnp.bfloat16)
    partial = jnp.dot(acted, narrow_weight, preferred_element_type=jnp.float32)
    return partial, (hidden, normed, inverse, hidden_low, pre_act, acted)


def ffn_backward(incoming, branch, kept, params):
    hidden, _, _, hidden_low, pre_act, acted = kept
    widen_weight, narrow_weight, second_gain, second_shift = (
        params[8],
        params[10],
        params[11],
        params[12],
    )
    result, normed, inverse = norm_forward(hidden + branch, second_gain, second_shift)
    grad_sum2, grad_gain, grad_shift = norm_backward(
        incoming.astype(jnp.float32), normed, inverse, second_gain
    )
    grad_branch = grad_sum2.astype(jnp.bfloat16)
    grad_acted = along_cols(grad_branch, narrow_weight)
    _, pull = jax.vjp(lambda value: jax.nn.gelu(value, approximate=True), pre_act)
    grad_pre = pull(grad_acted)[0].astype(jnp.bfloat16)
    partial = along_cols(grad_pre, widen_weight)
    narrow_total = over_rows(acted, grad_branch)
    widen_total = over_rows(hidden_low, grad_pre)
    bias_total = jnp.sum(grad_pre.astype(jnp.float32), axis=0)
    return partial, result, grad_sum2, (narrow_total, widen_total, bias_total, grad_gain, grad_shift)


def attn_backward(grad_hidden, inputs, box_low, pages, kept, norm_kept, params):
    query_cat, key_cat, values, mixed, totals = kept
    _, normed, inverse = norm_kept[:3]
    query_weight, key_weight, value_weight, out_weight, first_gain = (
        params[0],
        params[1],
        params[2],
        params[5],
        params[6],
    )
    grad_sum1, grad_gain, grad_shift = norm_backward(grad_hidden, normed, inverse, first_gain)
    grad_attended = grad_sum1.astype(jnp.bfloat16)
    grad_mixed = along_cols(grad_attended, out_weight).astype(jnp.bfloat16)
    grad_mixed = grad_mixed.reshape(values.shape)
    length = pages.shape[1]
    pieces = []
    for row in range(pages.shape[0]):
        pieces.append(
            attend_back(
                (query_cat[row], key_cat[row], values[row], grad_mixed[row], pages[row], totals[row])
            )
        )
    grad_qcat, grad_kcat, grad_vals = (
        jnp.concatenate([piece[i] for piece in pieces], axis=0) for i in range(3)
    )
    count = inputs.shape[0]
    gates = jnp.concatenate(
        [
            grad_qcat[..., :HEAD].reshape(count, -1),
            grad_kcat[..., :HEAD].reshape(count, -1),
            grad_vals.reshape(count, -1),
        ],
        axis=1,
    )
    box_gates = jnp.concatenate(
        [grad_qcat[..., HEAD:].reshape(count, -1), grad_kcat[..., HEAD:].reshape(count, -1)],
        axis=1,
    )
    partial = along_cols(
        gates, jnp.concatenate([query_weight, key_weight, value_weight], axis=1)
    )
    out_total = over_rows(grad_attended, jnp.concatenate(mixed, axis=0))
    return partial, grad_sum1, (
        out_total,
        over_rows(inputs, gates),
        over_rows(box_low, box_gates),
        grad_gain,
        grad_shift,
    )


def add_all(terms):
    return tuple(sum(parts[1:], parts[0]) for parts in zip(*terms))


def per_device(dp_count, *args):
    tokens, box_coords, page_lengths = args[:3]
    params = args[3:16]
    cotangent = args[16]
    rows = page_lengths.shape[0]
    length = tokens.shape[0] // rows
    width = tokens.shape[1]
    core = lax.axis_index("tp") % 2
    steps = rows // 2

    def arranged(value, step):
        flat = value.reshape(steps, 2, length, -1)[step]
        return jnp.where(core == 0, flat, flat[::-1]).reshape(2 * length, -1)

    lengths = page_lengths.reshape(steps, 2, -1)
    lengths = jnp.where(core == 0, lengths, lengths[:, ::-1])
    pages = [page_table(lengths[step], length) for step in range(steps)]
    coords = box_coords.reshape(2, steps, 2, length)
    coords = jnp.where(core == 0, coords, coords[:, :, ::-1])
    inputs = [arranged(tokens, step) for step in range(steps)]
    incoming = [arranged(cotangent, step) for step in range(steps)]
    boxes = [
        box_embed(coords[:, step].reshape(2, -1), width).astype(jnp.bfloat16)
        for step in range(steps)
    ]

    def restored(value):
        pair = value.reshape(2, length, width)
        return jnp.where(core == 0, pair, pair[::-1]).reshape(2 * length, width)

    previous = None

    def halved(parts):
        return parts[0] + trade_cores(parts[1])

    def arrived(half, then):
        whole = half + trade_chips(half)
        whole, then = lax.optimization_barrier((whole, then))
        return jnp.concatenate([whole, trade_cores(whole)], axis=0), then

    def pair(partial):
        return partial[:length], partial[length:]

    first, attn_kept = [], []
    for step in range(steps):
        given = inputs[step]
        if step:
            given, first[-1] = lax.optimization_barrier((given, first[-1]))
        parts, kept = attn_forward(given, boxes[step], pages[step], params)
        attn_kept.append(kept)
        first.append(halved(parts))
    second, ffn_kept = [], []
    for step in range(steps):
        latest = (first + second)[-1]
        attended, latest = arrived(first[step], latest)
        if step == 0:
            first[-1] = latest
        else:
            second[-1] = latest
        partial, kept = ffn_forward(inputs[step], attended, params)
        ffn_kept.append(kept)
        second.append(halved(pair(partial)))
    results, sums, third, ffn_terms = [], [], [], []
    for step in range(steps):
        latest = (second + third)[-1]
        branch, latest = arrived(second[step], latest)
        if step == 0:
            second[-1] = latest
        else:
            third[-1] = latest
        partial, result, grad_sum2, terms = ffn_backward(
            incoming[step], branch, ffn_kept[step], params
        )
        results.append(restored(result))
        ffn_terms.append(terms)
        sums.append(grad_sum2)
        third.append(halved(pair(partial)))
    narrow, widen, bias, second_gain, second_shift = add_all(ffn_terms)
    narrow = sum_over_dp(narrow, dp_count, (1, 2, 4))
    widen = sum_over_dp(widen, dp_count, (2, 1, 4))
    fourth, sums1, attn_terms = [], [], []
    for step in range(steps):
        latest = (third + fourth)[-1]
        back, latest = arrived(third[step], latest)
        if step == 0:
            third[-1] = latest
        else:
            fourth[-1] = latest
        partial, grad_sum1, terms = attn_backward(
            sums[step] + back,
            inputs[step],
            boxes[step],
            pages[step],
            attn_kept[step],
            ffn_kept[step][:3],
            params,
        )
        attn_terms.append(terms)
        sums1.append(grad_sum1)
        fourth.append(halved(pair(partial)))
    input_grads = []
    for step in range(steps):
        whole = fourth[step] + trade_chips(fourth[step])
        whole = jnp.concatenate([whole, trade_cores(whole)], axis=0)
        input_grads.append(restored(sums1[step] + whole))
    out_total, gates_total, box_total, first_gain, first_shift = add_all(attn_terms)
    out_total = sum_over_dp(out_total, dp_count, (2, 1, 4))
    gates_total = sum_over_dp(gates_total, dp_count, (1, 2, 4))
    box_total = sum_over_dp(box_total, dp_count, (2, 1, 4))
    small = jnp.stack([first_gain, first_shift, second_gain, second_shift, bias], axis=0)
    small = small_sum_over_dp(small, dp_count)
    own = params[0].shape[1]
    return (
        jnp.concatenate(results, axis=0),
        jnp.concatenate(input_grads, axis=0),
        gates_total[:, :own],
        gates_total[:, own : 2 * own],
        gates_total[:, 2 * own :],
        box_total[:, :own],
        box_total[:, own:],
        out_total.T,
        small[0],
        small[1],
        widen,
        small[4],
        narrow,
        small[2],
        small[3],
    )


def solution(mesh):
    placed = (
        P("dp", None),
        P(None, "dp"),
        P("dp", None),
        P(None, "tp"),
        P(None, "tp"),
        P(None, "tp"),
        P(None, "tp"),
        P(None, "tp"),
        P("tp", None),
        P(),
        P(),
        P(None, "tp"),
        P("tp"),
        P("tp", None),
        P(),
        P(),
        P("dp", None),
    )
    return jax.shard_map(
        functools.partial(per_device, mesh.shape["dp"]),
        mesh=mesh,
        in_specs=placed,
        out_specs=(
            P("dp", None),
            P("dp", None),
            P(None, "tp"),
            P(None, "tp"),
            P(None, "tp"),
            P(None, "tp"),
            P(None, "tp"),
            P("tp", None),
            P(),
            P(),
            P(None, "tp"),
            P("tp"),
            P("tp", None),
            P(),
            P(),
        ),
        check_vma=False,
    )
```
